32 devices in a mesh: row: 2 (over x), col: 16 (over z, y, core).
Axes of the slice: x: 2, y: 2, z: 4, core: 2. Of those that a mesh axis runs over, the one named last changes fastest.
Arguments:
- upper_a: float32 [8, 2, 256, 16, 256], P(None, 'row', None, 'col'), may hold values from -0.375 to 0.375
- upper_b: float32 [8, 2, 256, 16, 256], P(None, 'row', None, 'col'), may hold values from -0.375 to 0.375
- right_side: float32 [8, 2, 256, 16, 256], P(None, 'row', None, 'col'), may hold values from -6 to 6
- vectors_a: float32 [8, 2, 256, 256], P(None, 'row'), may hold values from -0.375 to 0.375
- inverse_a: float32 [8, 2, 256, 256], P(None, 'row'), may hold values from -0.375 to 0.375
- values_a: float32 [8, 2, 256], P(None, 'row'), may hold values from 0.5 to 2
- vectors_b: float32 [16, 256, 256], P('col'), may hold values from -0.375 to 0.375
- inverse_b: float32 [16, 256, 256], P('col'), may hold values from -0.375 to 0.375
- values_b: float32 [16, 256], P('col'), may hold values from 0.5 to 2
Outputs:
- solved: float32 [8, 2, 256, 16, 256], P(None, 'row', None, 'col')
The draws below stay inside these ranges and needn't reach their ends.
All inputs are finite; a program needn't handle non-finite values.
Results may differ from the reference program's by a relative error of at most 0.0001.
Values sent between devices are 32-bit elements; how exact they have to be, the bound alone decides.
A program may use at most 64 MiB of HBM per device.

```python
import math
import jax
import jax.numpy as jnp
from jax import lax

BLOCK = 256
FRONTS = 4
BLOCKS = 16
ROW_BLOCKS = 8
N_ROW = 2
N_COL = 16


def block_scale(own_key, shape, cuts, least, top_value):
    gain, own = 1.0, jax.random.fold_in(own_key, 6)
    for position, blocks in cuts:
        steps = jnp.exp(jax.random.uniform(jax.random.fold_in(own, position), (blocks,), jnp.float32, least / len(cuts), top_value / len(cuts)))
        gain = gain * jnp.repeat(steps, shape[position] // blocks).reshape([-1 if axis == position else 1 for axis in range(len(shape))])
    return gain


def normal_values(stream_key, shape, deviation, limit, cuts=(), kind=jnp.bfloat16):
    drawn = jax.random.normal(stream_key, shape, jnp.float32) * deviation
    if len(cuts) > 0:
        drawn = block_scale(stream_key, shape, cuts, -0.22, 0.18) * drawn
    return jnp.clip(drawn, min=-limit, max=limit).astype(kind)


def setup_inputs(seed: int = 0) -> dict:
    key_of = jax.random.split(jax.random.key(seed), 10)
    return {
        "upper_a": normal_values(key_of[0], (ROW_BLOCKS, N_ROW, BLOCK, N_COL, BLOCK), BLOCK ** -0.5, 0.375, ((1, 2), (3, 16)), jnp.float32),
        "upper_b": normal_values(key_of[1], (ROW_BLOCKS, N_ROW, BLOCK, N_COL, BLOCK), BLOCK ** -0.5, 0.375, ((1, 2), (3, 16)), jnp.float32),
        "right_side": normal_values(key_of[2], (ROW_BLOCKS, N_ROW, BLOCK, N_COL, BLOCK), 1.0, 6.0, ((1, 2), (3, 16)), jnp.float32),
        "vectors_a": normal_values(key_of[3], (ROW_BLOCKS, N_ROW, BLOCK, BLOCK), BLOCK ** -0.5, 0.375, ((1, 2),), jnp.float32),
        "inverse_a": normal_values(key_of[4], (ROW_BLOCKS, N_ROW, BLOCK, BLOCK), BLOCK ** -0.5, 0.375, ((1, 2),), jnp.float32),
        "values_a": jnp.clip(jnp.exp(math.log(2.0) - 1.3862944 * jax.random.uniform(key_of[5], (ROW_BLOCKS, N_ROW, BLOCK), jnp.float32) ** block_scale(key_of[5], (ROW_BLOCKS, N_ROW, BLOCK), ((1, 2),), -0.2, 0.2)), 0.5, 2.0),
        "vectors_b": normal_values(key_of[6], (BLOCKS, BLOCK, BLOCK), BLOCK ** -0.5, 0.375, ((0, 16),), jnp.float32),
        "inverse_b": normal_values(key_of[7], (BLOCKS, BLOCK, BLOCK), BLOCK ** -0.5, 0.375, ((0, 16),), jnp.float32),
        "values_b": jnp.clip(jnp.exp(math.log(2.0) - 1.3862944 * jax.random.uniform(key_of[8], (BLOCKS, BLOCK), jnp.float32) ** block_scale(key_of[8], (BLOCKS, BLOCK), ((0, 16),), -0.2, 0.2)), 0.5, 2.0),
    }


EXACT = lax.Precision.HIGHEST


def matmul(former, latter):
    return jnp.dot(former, latter, precision=EXACT, preferred_element_type=jnp.float32)


def diagonal_solve(residual, vectors_a, inverse_a, values_a, vectors_b, inverse_b, values_b):
    rotated = matmul(matmul(inverse_a, residual), vectors_b)
    scaled = rotated / (values_a[:, None] + values_b[None, :])
    return matmul(matmul(vectors_a, scaled), inverse_b)


def reference(upper_a, upper_b, right_side, vectors_a, inverse_a, values_a, vectors_b, inverse_b, values_b):
    block_grid = (BLOCKS, BLOCK, BLOCKS, BLOCK)
    matrix_a = upper_a.reshape(block_grid)
    matrix_b = upper_b.reshape(block_grid)
    work = right_side.reshape(block_grid)
    left_vectors = vectors_a.reshape(BLOCKS, BLOCK, BLOCK)
    left_inverse = inverse_a.reshape(BLOCKS, BLOCK, BLOCK)
    left_values = values_a.reshape(BLOCKS, BLOCK)
    block_ids = jnp.arange(BLOCKS, dtype=jnp.int32)
    diagonal_gap = block_ids[None, :] - block_ids[:, None]
    for front_step in range(FRONTS):
        offset = front_step - 1
        partner = block_ids + offset
        inside = (partner >= 0) & (partner < BLOCKS)
        partner_clip = jnp.clip(partner, 0, BLOCKS - 1).astype(jnp.int32)
        residual = work[block_ids, :, partner_clip, :]
        solved = jax.vmap(diagonal_solve)(residual, left_vectors, left_inverse, left_values,
                                          vectors_b[partner_clip], inverse_b[partner_clip], values_b[partner_clip])
        solved = jnp.where(inside[:, None, None], solved, jnp.zeros_like(solved))
        on_front = diagonal_gap == offset
        placed = solved[:, :, None, :] * on_front[:, None, :, None].astype(jnp.float32)
        work = jnp.where(on_front[:, None, :, None], placed, work)
        source = block_ids - offset
        source_valid = (source >= 0) & (source < BLOCKS)
        source_clip = jnp.clip(source, 0, BLOCKS - 1).astype(jnp.int32)
        column_solved = jnp.where(source_valid[:, None, None], solved[source_clip], jnp.zeros_like(solved))
        upper_panel = matrix_a[:, :, source_clip, :]
        upper_term = jnp.einsum("ixjy,jyz->ixjz", upper_panel, column_solved, precision=EXACT)
        lower_rows = matrix_b[partner_clip]
        lower_term = jnp.einsum("ixy,iyjz->ixjz", solved, lower_rows, precision=EXACT)
        pending = diagonal_gap > offset
        work = jnp.where(pending[:, None, :, None], work - (upper_term + lower_term), work)
    return work.reshape(right_side.shape)
```

```python
import functools

import jax
import jax.numpy as jnp
from jax import lax
from jax.experimental import pallas as pl
from jax.experimental.pallas import tpu as pltpu
from jax.sharding import PartitionSpec as P

FRONTS = 4
OFFSETS = tuple(range(-1, FRONTS - 1))
LAST = OFFSETS[-1]
MOVES = tuple(s for s in OFFSETS if s != 0)
EXACT = lax.Precision.HIGHEST
MESH = pl.DeviceIdType.MESH


def matmul(former, latter):
    return jnp.dot(former, latter, precision=EXACT, preferred_element_type=jnp.float32)


def split(value):
    high = value.astype(jnp.bfloat16)
    return high, (value - high.astype(jnp.float32)).astype(jnp.bfloat16)


def three(former, latter):
    fh, fl = split(former)
    lh, ll = split(latter)
    dot = functools.partial(jnp.dot, preferred_element_type=jnp.float32)
    return dot(fh, lh) + (dot(fh, ll) + dot(fl, lh))


def kernel(
    rows, cols, plane, turns, firsts,
    a_ref, b_ref, work_ref, va_ref, ia_ref, la_ref, vb_ref, ib_ref, lb_ref, out_ref,
    a_in, b_in, x_row, x_col,
    a_send, a_recv, b_send, b_recv, xc_send, xc_recv, xr_send, xr_recv,
):
    r = lax.axis_index("row")
    c = lax.axis_index("col")
    slots = a_ref.shape[0]
    total = slots * rows
    core = lax.rem(c, 2)
    place = lax.rem(c, plane)
    chips = plane // 2

    barrier = pltpu.get_barrier_semaphore()

    def greet_col(d, _):
        pl.semaphore_signal(barrier, inc=1, device_id=(r, lax.rem(c + d, cols)), device_id_type=MESH)
        return 0

    lax.fori_loop(1, cols, greet_col, 0)
    for d in range(1, rows):
        pl.semaphore_signal(barrier, inc=1, device_id=(lax.rem(r + d, rows), c), device_id_type=MESH)
    pl.semaphore_wait(barrier, cols - 1 + rows - 1)

    def remote(src, dst, send, recv, row, col):
        return pltpu.make_async_remote_copy(
            src_ref=src, dst_ref=dst, send_sem=send, recv_sem=recv,
            device_id=(row, col), device_id_type=MESH,
        )

    def a_copy(m, q):
        return remote(a_ref.at[q], a_in.at[m, q], a_send.at[m, q], a_recv.at[m, q],
                      r, lax.rem(c + MOVES[m] + cols, cols))

    def b_copy(d, q):
        to = lax.rem(r - turns[d] + rows, rows)
        return remote(b_ref.at[q], b_in.at[d, q], b_send.at[d, q], b_recv.at[d, q], to, c)

    def a_goes(m, q):
        to = c + MOVES[m]
        return (q * rows + r < c) & (to >= 0) & (to < cols)

    def b_goes(d, q):
        j = q * rows + r
        return (j < c) & (j - firsts[d] >= 0)

    def starts(step, _):
        q = slots - 1 - step
        for m in range(len(MOVES)):
            @pl.when(a_goes(m, q))
            def _():
                a_copy(m, q).start()
        for d in range(len(turns)):
            @pl.when(b_goes(d, q))
            def _():
                b_copy(d, q).start()
        return 0

    lax.fori_loop(0, slots, starts, 0)

    def front(s):
        i = c - s
        own = (i >= 0) & (i < total) & (lax.rem(i - r + rows, rows) == 0)
        q = jnp.clip((i - r + rows) // rows - 1, 0, slots - 1)
        return i, own, q

    def exists(s):
        return (c - s >= 0) & (c - s < total)

    def carrier(s):
        return lax.rem(r + s + 2 + core, 2) == 0

    def xc_copy(n, d):
        return remote(x_col.at[n], x_col.at[n], xc_send.at[n, d], xc_recv.at[n],
                      lax.rem(r + d, rows), c)

    def kind_to(kind):
        if kind == 0:
            return lax.rem(c + plane, cols)
        if kind == 1:
            return c + 1 - 2 * core
        return c - place + lax.rem(place + 2 * (kind - 1), plane)

    def kind_goes(n, q, kind):
        s = OFFSETS[n]
        i = q * rows + r
        c0 = i + s
        real = (c0 >= 0) & (c0 < cols) & carrier(s)
        mine = c0 == c
        below = c0 // plane < c // plane
        same = c0 // plane == c // plane
        to = kind_to(kind)
        holds = real & (mine | below | (same & (c0 >= 0)))
        if kind == 0:
            return holds & (c + plane < cols)
        if kind == 1:
            return holds & (to > c0)
        return real & mine & ((to > c0) | (c - place + plane < cols))

    def got(n, q):
        s = OFFSETS[n]
        c0 = q * rows + r + s
        real = (c0 >= 0) & (c0 < cols)
        same = c0 // plane == c // plane
        staged = same & carrier(s) & (c0 != c) & (c - place + plane < cols)
        return real & ((c0 < c) | staged)

    def xr_copy(n, q, kind, mine):
        src = x_col.at[n] if mine else x_row.at[n, q]
        return remote(src, x_row.at[n, q], xr_send.at[n, q, kind], xr_recv.at[n, q], r, kind_to(kind))

    kinds = [0, 1] + list(range(2, chips + 1))

    def take_a(m, q):
        a_copy(m, q).wait_recv()

    def take_x(n, q):
        xr_copy(n, q, 0, False).wait_recv()

    for n, s in enumerate(OFFSETS):
        i, own, q = front(s)

        @pl.when(own)
        def _(n=n, s=s, i=i, q=q):
            out_ref[q] = work_ref[q]
            for k in range(n):
                t = OFFSETS[k]

                @pl.when(exists(t))
                def _(k=k, t=t):
                    if t == 0:
                        part = a_ref.at[q]
                    else:
                        m = MOVES.index(t)
                        take_a(m, q)
                        part = a_in.at[m, q]
                    out_ref[q] = out_ref[q] - matmul(part[...], x_col[k])

                @pl.when(i + t >= 0)
                def _(k=k, t=t):
                    if (s - t) % 2 == 1:
                        take_x(k, q)
                    below = (i + t) // rows
                    turn = t % rows
                    if turn == 0:
                        part = b_ref.at[below]
                    else:
                        d = turns.index(turn)
                        if firsts[d] == t:
                            b_copy(d, below).wait_recv()
                        part = b_in.at[d, below]
                    out_ref[q] = out_ref[q] - matmul(x_row[k, q], part[...])

            rotated = matmul(matmul(ia_ref[q], out_ref[q]), vb_ref[...])
            scaled = rotated / (la_ref[q] + lb_ref[...])
            x_col[n] = matmul(matmul(va_ref[q], scaled), ib_ref[...])
            for d in range(1, rows):
                xc_copy(n, d).start()
            for kind in kinds:
                @pl.when(kind_goes(n, q, kind))
                def _(kind=kind):
                    xr_copy(n, q, kind, True).start()
            out_ref[q] = x_col[n]

        @pl.when(carrier(s))
        def _(n=n, s=s):
            def relay(step, _):
                q = slots - 1 - step

                @pl.when(got(n, q))
                def _():
                    take_x(n, q)
                    for kind in (0, 1):
                        @pl.when(kind_goes(n, q, kind))
                        def _(kind=kind):
                            xr_copy(n, q, kind, False).start()
                return 0

            lax.fori_loop(0, slots, relay, 0)

        @pl.when(exists(s) & jnp.logical_not(own))
        def _(n=n):
            xc_copy(n, 1).wait_recv()

    def finish(step, _):
        q = slots - 1 - step
        i = q * rows + r

        @pl.when(c - i > LAST)
        def _():
            out_ref[q] = work_ref[q]
            for n, s in enumerate(OFFSETS):
                @pl.when(exists(s))
                def _(n=n, s=s):
                    if s == 0:
                        part = a_ref.at[q]
                    else:
                        m = MOVES.index(s)
                        take_a(m, q)
                        part = a_in.at[m, q]
                    out_ref[q] = out_ref[q] - three(part[...], x_col[n])

                @pl.when(i + s >= 0)
                def _(n=n, s=s):
                    @pl.when(jnp.logical_not(carrier(s)))
                    def _():
                        take_x(n, q)
                    below = (i + s + rows) // rows - 1
                    turn = s % rows
                    if turn == 0:
                        part = b_ref.at[below]
                    else:
                        d = turns.index(turn)
                        if firsts[d] == s:
                            b_copy(d, below).wait_recv()
                        part = b_in.at[d, below]
                    out_ref[q] = out_ref[q] - three(x_row[n, q], part[...])

        @pl.when(c - i < OFFSETS[0])
        def _():
            out_ref[q] = work_ref[q]
        return 0

    lax.fori_loop(0, slots, finish, 0)

    def drain(q, _):
        for m in range(len(MOVES)):
            @pl.when(a_goes(m, q))
            def _():
                a_copy(m, q).wait_send()
        for d in range(len(turns)):
            @pl.when(b_goes(d, q))
            def _():
                b_copy(d, q).wait_send()
        for n in range(FRONTS):
            for kind in kinds:
                @pl.when(kind_goes(n, q, kind))
                def _():
                    xr_copy(n, q, kind, False).wait_send()
        return 0

    lax.fori_loop(0, slots, drain, 0)
    for n, s in enumerate(OFFSETS):
        _, own, _ = front(s)

        @pl.when(own)
        def _(n=n):
            for d in range(1, rows):
                xc_copy(n, d).wait_send()


def body(rows, cols, upper_a, upper_b, right_side, vectors_a, inverse_a, values_a, vectors_b, inverse_b, values_b):
    slots, size = right_side.shape[0], right_side.shape[2]
    square = (slots, size, size)
    turns, firsts = [], []
    for s in OFFSETS:
        if s % rows and s % rows not in turns:
            turns.append(s % rows)
            firsts.append(s)
    plane = max(2, cols // 4)
    moves, ways, kinds = len(MOVES), len(turns), plane // 2 + 1
    block = (size, size)
    out = pl.pallas_call(
        functools.partial(kernel, rows, cols, plane, tuple(turns), tuple(firsts)),
        out_shape=jax.ShapeDtypeStruct(square, jnp.float32),
        in_specs=[pl.BlockSpec(memory_space=pltpu.VMEM)] * 9,
        out_specs=pl.BlockSpec(memory_space=pltpu.VMEM),
        scratch_shapes=[
            pltpu.VMEM((moves, slots) + block, jnp.float32),
            pltpu.VMEM((ways, slots) + block, jnp.float32),
            pltpu.VMEM((FRONTS, slots) + block, jnp.float32),
            pltpu.VMEM((FRONTS,) + block, jnp.float32),
            pltpu.SemaphoreType.DMA((moves, slots)),
            pltpu.SemaphoreType.DMA((moves, slots)),
            pltpu.SemaphoreType.DMA((ways, slots)),
            pltpu.SemaphoreType.DMA((ways, slots)),
            pltpu.SemaphoreType.DMA((FRONTS, rows)),
            pltpu.SemaphoreType.DMA((FRONTS,)),
            pltpu.SemaphoreType.DMA((FRONTS, slots, kinds)),
            pltpu.SemaphoreType.DMA((FRONTS, slots)),
        ],
        compiler_params=pltpu.CompilerParams(
            collective_id=0, has_side_effects=True, vmem_limit_bytes=60 * 1024 * 1024
        ),
    )(
        upper_a.reshape(square), upper_b.reshape(square), right_side.reshape(square),
        vectors_a.reshape(square), inverse_a.reshape(square), values_a.reshape(slots, size, 1),
        vectors_b.reshape(block), inverse_b.reshape(block), values_b.reshape(1, size),
    )
    return out.reshape(right_side.shape)


def solution(mesh):
    return jax.shard_map(
        functools.partial(body, mesh.shape["row"], mesh.shape["col"]),
        mesh=mesh,
        in_specs=(
            P(None, "row", None, "col", None),
            P(None, "row", None, "col", None),
            P(None, "row", None, "col", None),
            P(None, "row", None, None),
            P(None, "row", None, None),
            P(None, "row", None),
            P("col", None, None),
            P("col", None, None),
            P("col", None),
        ),
        out_specs=P(None, "row", None, "col", None),
        check_vma=False,
    )
```

```python
import functools

import jax
import jax.numpy as jnp
from jax import lax
from jax.experimental import pallas as pl
from jax.experimental.pallas import tpu as pltpu
from jax.sharding import PartitionSpec as P

FRONTS = 4
OFFSETS = tuple(range(-1, FRONTS - 1))
LAST = OFFSETS[-1]
MOVES = tuple(s for s in OFFSETS if s != 0)
EXACT = lax.Precision.HIGHEST
MESH = pl.DeviceIdType.MESH


def matmul(former, latter):
    return jnp.dot(former, latter, precision=EXACT, preferred_element_type=jnp.float32)


def split(value):
    high = value.astype(jnp.bfloat16)
    return high, (value - high.astype(jnp.float32)).astype(jnp.bfloat16)


def three(former, latter):
    fh, fl = split(former)
    lh, ll = split(latter)
    dot = functools.partial(jnp.dot, preferred_element_type=jnp.float32)
    return dot(fh, lh) + (dot(fh, ll) + dot(fl, lh))


def kernel(
    rows, cols, plane, turns, firsts,
    a_ref, b_ref, work_ref, va_ref, ia_ref, la_ref, vb_ref, ib_ref, lb_ref, out_ref,
    a_in, b_in, x_row, x_col,
    a_send, a_recv, b_send, b_recv, xc_send, xc_recv, xr_send, xr_recv,
):
    r = lax.axis_index("row")
    c = lax.axis_index("col")
    slots = a_ref.shape[0]
    total = slots * rows
    core = lax.rem(c, 2)
    place = lax.rem(c, plane)
    chips = plane // 2

    barrier = pltpu.get_barrier_semaphore()

    def greet_col(d, _):
        pl.semaphore_signal(barrier, inc=1, device_id=(r, lax.rem(c + d, cols)), device_id_type=MESH)
        return 0

    lax.fori_loop(1, cols, greet_col, 0)
    for d in range(1, rows):
        pl.semaphore_signal(barrier, inc=1, device_id=(lax.rem(r + d, rows), c), device_id_type=MESH)
    pl.semaphore_wait(barrier, cols - 1 + rows - 1)

    def remote(src, dst, send, recv, row, col):
        return pltpu.make_async_remote_copy(
            src_ref=src, dst_ref=dst, send_sem=send, recv_sem=recv,
            device_id=(row, col), device_id_type=MESH,
        )

    def a_copy(m, q):
        return remote(a_ref.at[q], a_in.at[m, q], a_send.at[m, q], a_recv.at[m, q],
                      r, lax.rem(c + MOVES[m] + cols, cols))

    def b_copy(d, q):
        to = lax.rem(r - turns[d] + rows, rows)
        return remote(b_ref.at[q], b_in.at[d, q], b_send.at[d, q], b_recv.at[d, q], to, c)

    def a_goes(m, q):
        to = c + MOVES[m]
        return (q * rows + r < c) & (to >= 0) & (to < cols)

    def b_goes(d, q):
        j = q * rows + r
        return (j < c) & (j - firsts[d] >= 0)

    near = LAST - OFFSETS[0]
    bounds = (0, near + 1, near + 1 + 3 * cols // 8, total + cols)

    def starts(part):
        def one(step, _):
            q = slots - 1 - step
            gap = c - (q * rows + r)
            now = (gap >= bounds[part]) & (gap < bounds[part + 1])
            for m in range(len(MOVES)):
                @pl.when(now & a_goes(m, q))
                def _(m=m):
                    a_copy(m, q).start()
            for d in range(len(turns)):
                @pl.when(now & b_goes(d, q))
                def _(d=d):
                    b_copy(d, q).start()
            return 0

        lax.fori_loop(0, slots, one, 0)

    starts(0)

    def front(s):
        i = c - s
        own = (i >= 0) & (i < total) & (lax.rem(i - r + rows, rows) == 0)
        q = jnp.clip((i - r + rows) // rows - 1, 0, slots - 1)
        return i, own, q

    def exists(s):
        return (c - s >= 0) & (c - s < total)

    def carrier(s):
        return lax.rem(r + s + 2 + core, 2) == 0

    def xc_copy(n, d):
        return remote(x_col.at[n], x_col.at[n], xc_send.at[n, d], xc_recv.at[n],
                      lax.rem(r + d, rows), c)

    def kind_to(kind):
        if kind == 0:
            return lax.rem(c + plane, cols)
        if kind == 1:
            return c + 1 - 2 * core
        return c - place + lax.rem(place + 2 * (kind - 1), plane)

    def kind_goes(n, q, kind):
        s = OFFSETS[n]
        i = q * rows + r
        c0 = i + s
        real = (c0 >= 0) & (c0 < cols) & carrier(s)
        mine = c0 == c
        below = c0 // plane < c // plane
        same = c0 // plane == c // plane
        to = kind_to(kind)
        holds = real & (mine | below | (same & (c0 >= 0)))
        if kind == 0:
            return holds & (c + plane < cols)
        if kind == 1:
            return holds & (to > c0)
        return real & mine & ((to > c0) | (c - place + plane < cols))

    def got(n, q):
        s = OFFSETS[n]
        c0 = q * rows + r + s
        real = (c0 >= 0) & (c0 < cols)
        same = c0 // plane == c // plane
        staged = same & carrier(s) & (c0 != c) & (c - place + plane < cols)
        return real & ((c0 < c) | staged)

    def xr_copy(n, q, kind, mine):
        src = x_col.at[n] if mine else x_row.at[n, q]
        return remote(src, x_row.at[n, q], xr_send.at[n, q, kind], xr_recv.at[n, q], r, kind_to(kind))

    kinds = [0, 1] + list(range(2, chips + 1))

    def take_a(m, q):
        a_copy(m, q).wait_recv()

    def take_x(n, q):
        xr_copy(n, q, 0, False).wait_recv()

    for n, s in enumerate(OFFSETS):
        i, own, q = front(s)

        @pl.when(own)
        def _(n=n, s=s, i=i, q=q):
            out_ref[q] = work_ref[q]
            for k in range(n):
                t = OFFSETS[k]

                @pl.when(exists(t))
                def _(k=k, t=t):
                    if t == 0:
                        part = a_ref.at[q]
                    else:
                        m = MOVES.index(t)
                        take_a(m, q)
                        part = a_in.at[m, q]
                    out_ref[q] = out_ref[q] - matmul(part[...], x_col[k])

                @pl.when(i + t >= 0)
                def _(k=k, t=t):
                    if (s - t) % 2 == 1:
                        take_x(k, q)
                    below = (i + t) // rows
                    turn = t % rows
                    if turn == 0:
                        part = b_ref.at[below]
                    else:
                        d = turns.index(turn)
                        if firsts[d] == t:
                            b_copy(d, below).wait_recv()
                        part = b_in.at[d, below]
                    out_ref[q] = out_ref[q] - matmul(x_row[k, q], part[...])

            rotated = matmul(matmul(ia_ref[q], out_ref[q]), vb_ref[...])
            scaled = rotated / (la_ref[q] + lb_ref[...])
            x_col[n] = matmul(matmul(va_ref[q], scaled), ib_ref[...])
            for d in range(1, rows):
                xc_copy(n, d).start()
            for kind in kinds:
                @pl.when(kind_goes(n, q, kind))
                def _(kind=kind):
                    xr_copy(n, q, kind, True).start()
            out_ref[q] = x_col[n]

        @pl.when(carrier(s))
        def _(n=n, s=s):
            starts(1 + n // 2)

            def relay(step, _):
                q = slots - 1 - step

                @pl.when(got(n, q))
                def _():
                    take_x(n, q)
                    for kind in (0, 1):
                        @pl.when(kind_goes(n, q, kind))
                        def _(kind=kind):
                            xr_copy(n, q, kind, False).start()
                return 0

            lax.fori_loop(0, slots, relay, 0)

        @pl.when(exists(s) & jnp.logical_not(own))
        def _(n=n):
            xc_copy(n, 1).wait_recv()

    def finish(step, _):
        q = slots - 1 - step
        i = q * rows + r

        @pl.when(c - i > LAST)
        def _():
            out_ref[q] = work_ref[q]
            for n, s in enumerate(OFFSETS):
                @pl.when(exists(s))
                def _(n=n, s=s):
                    if s == 0:
                        part = a_ref.at[q]
                    else:
                        m = MOVES.index(s)
                        take_a(m, q)
                        part = a_in.at[m, q]
                    out_ref[q] = out_ref[q] - three(part[...], x_col[n])

                @pl.when(i + s >= 0)
                def _(n=n, s=s):
                    @pl.when(jnp.logical_not(carrier(s)))
                    def _():
                        take_x(n, q)
                    below = (i + s + rows) // rows - 1
                    turn = s % rows
                    if turn == 0:
                        part = b_ref.at[below]
                    else:
                        d = turns.index(turn)
                        if firsts[d] == s:
                            b_copy(d, below).wait_recv()
                        part = b_in.at[d, below]
                    out_ref[q] = out_ref[q] - three(x_row[n, q], part[...])

        @pl.when(c - i < OFFSETS[0])
        def _():
            out_ref[q] = work_ref[q]
        return 0

    lax.fori_loop(0, slots, finish, 0)

    def drain(q, _):
        for m in range(len(MOVES)):
            @pl.when(a_goes(m, q))
            def _():
                a_copy(m, q).wait_send()
        for d in range(len(turns)):
            @pl.when(b_goes(d, q))
            def _():
                b_copy(d, q).wait_send()
        for n in range(FRONTS):
            for kind in kinds:
                @pl.when(kind_goes(n, q, kind))
                def _():
                    xr_copy(n, q, kind, False).wait_send()
        return 0

    lax.fori_loop(0, slots, drain, 0)
    for n, s in enumerate(OFFSETS):
        _, own, _ = front(s)

        @pl.when(own)
        def _(n=n):
            for d in range(1, rows):
                xc_copy(n, d).wait_send()


def body(rows, cols, upper_a, upper_b, right_side, vectors_a, inverse_a, values_a, vectors_b, inverse_b, values_b):
    slots, size = right_side.shape[0], right_side.shape[2]
    square = (slots, size, size)
    turns, firsts = [], []
    for s in OFFSETS:
        if s % rows and s % rows not in turns:
            turns.append(s % rows)
            firsts.append(s)
    plane = max(2, cols // 4)
    moves, ways, kinds = len(MOVES), len(turns), plane // 2 + 1
    block = (size, size)
    out = pl.pallas_call(
        functools.partial(kernel, rows, cols, plane, tuple(turns), tuple(firsts)),
        out_shape=jax.ShapeDtypeStruct(square, jnp.float32),
        in_specs=[pl.BlockSpec(memory_space=pltpu.VMEM)] * 9,
        out_specs=pl.BlockSpec(memory_space=pltpu.VMEM),
        scratch_shapes=[
            pltpu.VMEM((moves, slots) + block, jnp.float32),
            pltpu.VMEM((ways, slots) + block, jnp.float32),
            pltpu.VMEM((FRONTS, slots) + block, jnp.float32),
            pltpu.VMEM((FRONTS,) + block, jnp.float32),
            pltpu.SemaphoreType.DMA((moves, slots)),
            pltpu.SemaphoreType.DMA((moves, slots)),
            pltpu.SemaphoreType.DMA((ways, slots)),
            pltpu.SemaphoreType.DMA((ways, slots)),
            pltpu.SemaphoreType.DMA((FRONTS, rows)),
            pltpu.SemaphoreType.DMA((FRONTS,)),
            pltpu.SemaphoreType.DMA((FRONTS, slots, kinds)),
            pltpu.SemaphoreType.DMA((FRONTS, slots)),
        ],
        compiler_params=pltpu.CompilerParams(
            collective_id=0, has_side_effects=True, vmem_limit_bytes=60 * 1024 * 1024
        ),
    )(
        upper_a.reshape(square), upper_b.reshape(square), right_side.reshape(square),
        vectors_a.reshape(square), inverse_a.reshape(square), values_a.reshape(slots, size, 1),
        vectors_b.reshape(block), inverse_b.reshape(block), values_b.reshape(1, size),
    )
    return out.reshape(right_side.shape)


def solution(mesh):
    return jax.shard_map(
        functools.partial(body, mesh.shape["row"], mesh.shape["col"]),
        mesh=mesh,
        in_specs=(
            P(None, "row", None, "col", None),
            P(None, "row", None, "col", None),
            P(None, "row", None, "col", None),
            P(None, "row", None, None),
            P(None, "row", None, None),
            P(None, "row", None),
            P("col", None, None),
            P("col", None, None),
            P("col", None),
        ),
        out_specs=P(None, "row", None, "col", None),
        check_vma=False,
    )
```
